32 devices in a mesh: bank: 4 (over z), zero: 8 (over y, x, core).
Axes of the slice: x: 2, y: 2, z: 4, core: 2. Of those that a mesh axis runs over, the one named last changes fastest.
Arguments:
- train_gate: float32 [64, 2048, 1408], P('bank', 'zero'), may hold values from -0.1875 to 0.1875
- train_up: float32 [64, 2048, 1408], P('bank', 'zero'), may hold values from -0.1875 to 0.1875
- router_weight: float32 [2048, 64], P('zero', 'bank'), may hold values from -0.125 to 0.125
- router_gain: float32 [2048], P('zero'), may hold values from 0.25 to 1.75
Outputs:
- ready_gate: bfloat16 [64, 2048, 1408], P('bank', None, 'zero')
- ready_up: bfloat16 [64, 2048, 1408], P('bank', None, 'zero')
- scale_gate: float32 [64, 1408], P('bank', 'zero')
- scale_up: float32 [64, 1408], P('bank', 'zero')
- serve_router: bfloat16 [2048, 64], replicated
The draws below stay inside these ranges and needn't reach their ends.
All inputs are finite; a program needn't handle non-finite values. Where the reference program divides by a largest or mean magnitude, that divisor is 1e-20 or more.
Results may differ from the reference program's by a relative error of at most 0.012.
Values may be sent and summed in bfloat16 or wider, within the bound.
A program may use at most 192 MiB of HBM per device.

```python
import jax
import jax.numpy as jnp

EXPERTS = 64
D_MODEL = 2048
D_EXPERT = 1408


def spiked(result, key, source, target, blocks, factor):
    def block_of(axis_at):
        return (jnp.arange(result.shape[axis_at]) // (result.shape[axis_at] // blocks)).reshape((-1,) + (1,) * (result.ndim - 1 - axis_at))

    one_side = jax.random.permutation(key, blocks)[block_of(target)]
    other_side = (block_of(target) + blocks // 2) % blocks
    return jnp.where((block_of(source) == one_side) | (block_of(source) == other_side), factor * result, result)


def level_of(own_key, dims, pieces, low, top_value):
    def one(position, shards_of):
        steps = jax.random.uniform(jax.random.fold_in(jax.random.fold_in(own_key, 6), position), (shards_of,), jnp.float32, low / len(pieces), top_value / len(pieces))
        return jnp.repeat(jnp.exp(steps), dims[position] // shards_of).reshape((-1,) + (1,) * (len(dims) - position - 1))

    loudness = one(*pieces[0])
    for cut in pieces[1:]:
        loudness = loudness * one(*cut)
    return loudness


def gaussian(stream_key, dims, deviation, reach, pieces=(), dtype=jnp.bfloat16):
    values = jax.random.normal(stream_key, dims, jnp.float32) * deviation
    if len(pieces) > 0:
        values = level_of(stream_key, dims, pieces, -0.22, 0.18) * values
    return jnp.clip(values, min=-reach, max=reach).astype(dtype)


def noise_with(key, shape, spread, limit, cuts, heavy, kind=jnp.bfloat16):
    drawn = spread * jax.random.normal(key, shape, jnp.float32)
    if cuts:
        drawn = drawn * level_of(key, shape, cuts, -0.22, 0.18)
    return jnp.clip(spiked(drawn, jax.random.fold_in(key, 3), *heavy), -limit, limit).astype(kind)


def setup_inputs(seed: int = 0) -> dict:
    key_list = jax.random.split(jax.random.key(seed), 5)
    return {
        "train_gate": noise_with(key_list[0], (EXPERTS, D_MODEL, D_EXPERT), D_MODEL ** -0.5, 0.1875, ((0, 4), (1, 8)), (1, 2, 8, 2.0), jnp.float32),
        "train_up": noise_with(key_list[1], (EXPERTS, D_MODEL, D_EXPERT), D_MODEL ** -0.5, 0.1875, ((0, 4), (1, 8)), (1, 2, 8, 2.0), jnp.float32),
        "router_weight": gaussian(key_list[2], (D_MODEL, EXPERTS), D_MODEL ** -0.5, 0.125, ((0, 8), (1, 4)), jnp.float32),
        "router_gain": jnp.clip(1.0 + 0.15 * jax.random.normal(key_list[3], (D_MODEL,), jnp.float32), 0.25, 1.75),
    }


def reference(train_gate, train_up, router_weight, router_gain):
    scale_gate = jnp.sum(jnp.abs(train_gate), axis=1) / D_MODEL
    ready_gate = (train_gate / jnp.expand_dims(scale_gate, 1)).astype(jnp.bfloat16)
    scale_up = jnp.sum(jnp.abs(train_up), axis=1) / D_MODEL
    ready_up = (train_up / jnp.expand_dims(scale_up, 1)).astype(jnp.bfloat16)
    serve_router = (router_weight * router_gain[:, None]).astype(jnp.bfloat16)
    return ready_gate, ready_up, scale_gate, scale_up, serve_router
```

```python
import functools

import jax
import jax.numpy as jnp
from jax import lax
from jax.experimental import pallas as pl
from jax.experimental.pallas import tpu as pltpu
from jax.sharding import PartitionSpec as P

MESH = pl.DeviceIdType.MESH
LANES = 128
SLOTS = 8
LAG = 5
KERNEL_VMEM = 28 * 2**20
FINISH_VMEM = 2 * 2**20


def exchange(
    n, nb, gate, up, weight, gain, recv, router, scale_gate, scale_up, inbuf, turned, send, part, wide,
    weight_buf, gain_buf, in_sem, router_sem, send_sem, recv_sem, bank_send, bank_recv, zero_send, zero_recv,
):
    experts, rows, cols = gate.shape
    width = cols // n
    steps = 2 * experts
    slots = send.shape[0]
    lag = min(LAG, experts)
    me = lax.axis_index("zero")
    bank = lax.axis_index("bank")

    def fetch(source, e, slot):
        return pltpu.make_async_copy(source.at[e], inbuf.at[slot], in_sem.at[slot])

    router_in = (
        pltpu.make_async_copy(weight, weight_buf, router_sem.at[0]),
        pltpu.make_async_copy(gain, gain_buf, router_sem.at[1]),
    )

    fetch(gate, 0, 0).start()
    for copy in router_in:
        copy.start()
    fetch(up, 0, 1).start()

    barrier = pltpu.get_barrier_semaphore()
    for k in range(1, n):
        pl.semaphore_signal(barrier, inc=1, device_id={"zero": lax.rem(me + k, n)}, device_id_type=MESH)
    for k in range(1, nb):
        pl.semaphore_signal(barrier, inc=1, device_id={"bank": lax.rem(bank + k, nb)}, device_id_type=MESH)
    scale_gate[...] = jnp.zeros_like(scale_gate)
    scale_up[...] = jnp.zeros_like(scale_up)

    def peer_copy(half, e, slot, k):
        peer = lax.rem(me + k, n)
        return pltpu.make_async_remote_copy(
            src_ref=send.at[slot, peer],
            dst_ref=recv.at[me, half, e],
            send_sem=send_sem.at[slot, k],
            recv_sem=recv_sem.at[2 * e + half, k],
            device_id={"zero": peer},
            device_id_type=MESH,
        )

    def turn(half, slot):
        for j in range(0, cols, LANES):
            turned[j : j + LANES, :] = inbuf[half, :, j : j + LANES].T
        for d in range(n):
            send[slot, d] = turned[d * width : (d + 1) * width, :].astype(send.dtype)

    def drain(slot):
        for k in range(1, n):
            peer_copy(0, 0, slot, k).wait_send()

    def launch(half, e, slot):
        for k in range(1, n):
            peer_copy(half, e, slot, k).start()
        recv[me, half, e] = send[slot, me]

    def settle(half, scale, e):
        total = jnp.zeros((width, LANES), jnp.float32)
        for k in range(n):
            source = lax.rem(me - k + n, n)
            block = recv.at[source, half, e]
            if k > 0:
                pltpu.make_async_remote_copy(
                    src_ref=block,
                    dst_ref=block,
                    send_sem=send_sem.at[0, 0],
                    recv_sem=recv_sem.at[2 * e + half, k],
                    device_id={"zero": source},
                    device_id_type=MESH,
                ).wait_recv()
            for j in range(0, rows, LANES):
                total += jnp.abs(block[:, j : j + LANES].astype(jnp.float32))
        mean = jnp.sum(total, axis=1, keepdims=True) / (rows * n)
        wide[0:width, :] = jnp.broadcast_to(mean, (width, LANES))
        for j in range(0, width, LANES):
            stop = min(j + LANES, width)
            line = wide[j : j + LANES, :].T[0:1, 0 : stop - j]
            here = lax.broadcasted_iota(jnp.int32, (experts, stop - j), 0) == e
            scale[:, j:stop] = jnp.where(here, line, scale[:, j:stop])
        inverse = jnp.broadcast_to(1.0 / mean, (width, LANES))
        for s in range(n):
            for j in range(0, rows, LANES):
                value = recv[s, half, e, :, j : j + LANES].astype(jnp.float32) * inverse
                recv[s, half, e, :, j : j + LANES] = value.astype(recv.dtype)

    def settle_both(e):
        for half, scale in enumerate((scale_gate, scale_up)):
            settle(half, scale, e)

    def column(z):
        return pl.ds(pl.multiple_of(z * rows, rows), rows)

    def bank_copy(k):
        return pltpu.make_async_remote_copy(
            src_ref=part,
            dst_ref=router.at[bank, :, column(me)],
            send_sem=bank_send.at[k],
            recv_sem=bank_recv.at[k],
            device_id={"bank": lax.rem(bank + k, nb)},
            device_id_type=MESH,
        )

    def zero_copy(k):
        return pltpu.make_async_remote_copy(
            src_ref=router.at[:, :, column(me)],
            dst_ref=router.at[:, :, column(me)],
            send_sem=zero_send.at[k],
            recv_sem=zero_recv.at[k],
            device_id={"zero": lax.rem(me + k, n)},
            device_id_type=MESH,
        )

    fetch(gate, 0, 0).wait()
    turn(0, 0)
    pl.semaphore_wait(barrier, n - 1 + nb - 1)

    launch(0, 0, 0)

    for copy in router_in:
        copy.wait()
    part[...] = (weight_buf[...] * gain_buf[...]).astype(part.dtype)
    router[bank, :, column(me)] = part[...]
    for k in range(1, nb):
        bank_copy(k).start()

    @pl.loop(0, experts)
    def _(e):
        for half, source in enumerate((gate, up)):
            t = 2 * e + half
            slot = lax.rem(t, slots)

            def ready():
                fetch(source, e, half).wait()

                @pl.when(t >= slots)
                def _():
                    drain(slot)

                turn(half, slot)

                launch(half, e, slot)

            if half == 0:
                pl.when(e > 0)(ready)
            else:
                ready()

            @pl.when(e + 1 < experts)
            def _():
                fetch(source, e + 1, half).start()

        @pl.when(e == min(1, experts - 1))
        def _():
            for k in range(1, nb):
                bank_copy(k).wait()
            for k in range(1, n):
                zero_copy(k).start()

        @pl.when(e >= lag)
        def _():
            settle_both(e - lag)

    @pl.loop(experts - lag, experts)
    def _(e):
        settle_both(e)

    for k in range(1, n):
        zero_copy(k).wait()

    @pl.loop(max(steps - slots, 0), steps)
    def _(t):
        drain(lax.rem(t, slots))


def finish(
    recv, router, scale_gate, scale_up,
    ready_gate, ready_up, router_out, scale_gate_out, scale_up_out, sem, small_sem,
):
    n, rows = recv.shape[0], recv.shape[4]
    copies = [
        pltpu.make_async_copy(recv.at[s, half], ready.at[:, :, s * rows : (s + 1) * rows], sem.at[s, half])
        for s in range(n)
        for half, ready in enumerate((ready_gate, ready_up))
    ]
    copies += [
        pltpu.make_async_copy(router, router_out, small_sem.at[0]),
        pltpu.make_async_copy(scale_gate, scale_gate_out, small_sem.at[1]),
        pltpu.make_async_copy(scale_up, scale_up_out, small_sem.at[2]),
    ]
    for copy in copies:
        copy.start()
    for copy in copies:
        copy.wait()


def solution(mesh):
    n, nb = mesh.shape["zero"], mesh.shape["bank"]

    def local(train_gate, train_up, router_weight, router_gain):
        experts, rows, cols = train_gate.shape
        width = cols // n
        d_model = rows * n
        mine = router_weight.shape[1]
        slots = min(SLOTS, 2 * experts)
        hbm = pl.BlockSpec(memory_space=pltpu.HBM)
        inside = pl.BlockSpec(memory_space=pltpu.VMEM)
        padded = -(-width // LANES) * LANES
        scale = jax.ShapeDtypeStruct((experts, width), jnp.float32)
        joined = jax.ShapeDtypeStruct((nb, mine, d_model), jnp.bfloat16)
        recv, router, scale_gate, scale_up = pl.pallas_call(
            functools.partial(exchange, n, nb),
            out_shape=(
                jax.ShapeDtypeStruct((n, 2, experts, width, rows), jnp.bfloat16),
                joined,
                scale,
                scale,
            ),
            in_specs=[hbm] * 4,
            out_specs=(inside,) * 4,
            scratch_shapes=[
                pltpu.VMEM((2, rows, cols), jnp.float32),
                pltpu.VMEM((cols, rows), jnp.float32),
                pltpu.VMEM((slots, n, width, rows), jnp.bfloat16),
                pltpu.VMEM((mine, rows), jnp.bfloat16),
                pltpu.VMEM((padded, LANES), jnp.float32),
                pltpu.VMEM((mine, rows), jnp.float32),
                pltpu.VMEM((1, rows), jnp.float32),
                pltpu.SemaphoreType.DMA((2,)),
                pltpu.SemaphoreType.DMA((2,)),
                pltpu.SemaphoreType.DMA((slots, n)),
                pltpu.SemaphoreType.DMA((2 * experts, n)),
                pltpu.SemaphoreType.DMA((nb,)),
                pltpu.SemaphoreType.DMA((nb,)),
                pltpu.SemaphoreType.DMA((n,)),
                pltpu.SemaphoreType.DMA((n,)),
            ],
            compiler_params=pltpu.CompilerParams(
                collective_id=0, has_side_effects=True, vmem_limit_bytes=KERNEL_VMEM
            ),
        )(
            train_gate,
            train_up,
            pltpu.with_memory_space_constraint(router_weight.T, pltpu.HBM),
            pltpu.with_memory_space_constraint(router_gain[None, :], pltpu.HBM),
        )

        ready = jax.ShapeDtypeStruct((experts, width, d_model), jnp.bfloat16)
        ready_gate, ready_up, router, scale_gate, scale_up = pl.pallas_call(
            finish,
            out_shape=(ready, ready, joined, scale, scale),
            in_specs=[inside] * 4,
            out_specs=(hbm,) * 5,
            scratch_shapes=[pltpu.SemaphoreType.DMA((n, 2)), pltpu.SemaphoreType.DMA((3,))],
            compiler_params=pltpu.CompilerParams(vmem_limit_bytes=FINISH_VMEM),
        )(recv, router, scale_gate, scale_up)
        return (
            jnp.swapaxes(ready_gate, 1, 2),
            jnp.swapaxes(ready_up, 1, 2),
            scale_gate,
            scale_up,
            router.reshape(nb * mine, d_model).T,
        )

    in_specs = (P("bank", "zero", None), P("bank", "zero", None), P("zero", "bank"), P("zero"))
    out_specs = (
        P("bank", None, "zero"),
        P("bank", None, "zero"),
        P("bank", "zero"),
        P("bank", "zero"),
        P(),
    )
    return jax.shard_map(local, mesh=mesh, in_specs=in_specs, out_specs=out_specs, check_vma=False)
```

```python
import functools

import jax
import jax.numpy as jnp
from jax import lax
from jax.experimental import pallas as pl
from jax.experimental.pallas import tpu as pltpu
from jax.sharding import PartitionSpec as P

MESH = pl.DeviceIdType.MESH
LANES = 128
SLOTS = 8
LAG = 5
TAIL = 3 / 16
EXCHANGE_VMEM = 28 * 2**20
CROSS_VMEM = 8 * 2**20
FINISH_VMEM = 2 * 2**20


def at(axis, index):
    return dict(device_id={axis: index}, device_id_type=MESH)


def spread(mean, wide, scale, row):
    width = mean.shape[0]
    wide[0:width, :] = jnp.broadcast_to(mean, (width, LANES))
    for j in range(0, width, LANES):
        stop = min(j + LANES, width)
        line = wide[j : j + LANES, :].T[0:1, 0 : stop - j]
        here = lax.broadcasted_iota(jnp.int32, (scale.shape[0], stop - j), 0) == row
        scale[:, j:stop] = jnp.where(here, line, scale[:, j:stop])


def settle(n, blocks, arrive, wide, scale, row):
    width, rows = blocks(0).shape
    total = jnp.zeros((width, LANES), jnp.float32)
    for k in range(n):
        arrive(k)
        block = blocks(k)
        for j in range(0, rows, LANES):
            total += jnp.abs(block[:, j : j + LANES].astype(jnp.float32))
    mean = jnp.sum(total, axis=1, keepdims=True) / (rows * n)
    inverse = jnp.broadcast_to(1.0 / mean, (width, LANES))
    for k in range(n):
        block = blocks(k)
        for j in range(0, rows, LANES):
            value = block[:, j : j + LANES].astype(jnp.float32) * inverse
            block[:, j : j + LANES] = value.astype(block.dtype)
    spread(mean, wide, scale, row)


def exchange(
    n, nb, gate, up, weight, gain, recv, router, scale_gate, scale_up, late, early,
    inbuf, turned, send, part, wide, weight_buf, gain_buf,
    in_sem, router_sem, send_sem, recv_sem, late_send, late_recv,
    bank_send, bank_recv, zero_send, zero_recv, here_sem, go_sem,
):
    experts, rows, cols = gate.shape
    width = cols // n
    bulk = recv.shape[2]
    slots = send.shape[0]
    lag = min(LAG, bulk)
    me = lax.axis_index("zero")
    bank = lax.axis_index("bank")
    odd = lax.rem(me, 2) == 1

    def fetch(source, e, slot):
        return pltpu.make_async_copy(source.at[e], inbuf.at[slot], in_sem.at[slot])

    router_in = (
        pltpu.make_async_copy(weight, weight_buf, router_sem.at[0]),
        pltpu.make_async_copy(gain, gain_buf, router_sem.at[1]),
    )

    fetch(gate, 0, 0).start()

    barrier = pltpu.get_barrier_semaphore()
    for k in range(1, n):
        peer = lax.rem(me + k, n)

        @pl.when(peer != 0)
        def _():
            pl.semaphore_signal(barrier, inc=1, **at("zero", peer))

    for copy in router_in:
        copy.start()
    scale_gate[...] = jnp.zeros_like(scale_gate)
    scale_up[...] = jnp.zeros_like(scale_up)

    def peer_copy(half, e, slot, k):
        peer = lax.rem(me + k, n)
        return pltpu.make_async_remote_copy(
            src_ref=send.at[slot, peer],
            dst_ref=recv.at[me, half, e],
            send_sem=send_sem.at[slot, k],
            recv_sem=recv_sem.at[2 * e + half, k],
            **at("zero", peer),
        )

    def late_copy(half, e, k):
        peer = lax.rem(me + k, n)
        return pltpu.make_async_remote_copy(
            src_ref=late.at[peer, half, e],
            dst_ref=early.at[me // 2, half, e],
            send_sem=late_send.at[2 * e + half, k],
            recv_sem=late_recv.at[2 * e + half, k],
            **at("zero", peer),
        )

    def turn(half, target):
        for j in range(0, cols, LANES):
            turned[j : j + LANES, :] = inbuf[half, :, j : j + LANES].T
        for d in range(n):
            target(d)[...] = turned[d * width : (d + 1) * width, :].astype(send.dtype)

    def drain(slot):
        for k in range(1, n):
            peer_copy(0, 0, slot, k).wait_send()

    def launch(half, e, slot):
        for k in range(1, n):
            peer_copy(half, e, slot, k).start()
        recv[me, half, e] = send[slot, me]

    def settle_both(e):
        for half, scale in enumerate((scale_gate, scale_up)):

            def block(k):
                return recv.at[lax.rem(me - k + n, n), half, e]

            def arrive(k):
                if k > 0:
                    pltpu.make_async_remote_copy(
                        src_ref=block(k),
                        dst_ref=block(k),
                        send_sem=send_sem.at[0, 0],
                        recv_sem=recv_sem.at[2 * e + half, k],
                        **at("zero", lax.rem(me - k + n, n)),
                    ).wait_recv()

            settle(n, block, arrive, wide, scale, e)

    def column(z):
        return pl.ds(pl.multiple_of(z * rows, rows), rows)

    def bank_copy(k):
        return pltpu.make_async_remote_copy(
            src_ref=part,
            dst_ref=router.at[bank, :, column(me)],
            send_sem=bank_send.at[k],
            recv_sem=bank_recv.at[k],
            **at("bank", lax.rem(bank + k, nb)),
        )

    def zero_copy(k):
        return pltpu.make_async_remote_copy(
            src_ref=router.at[:, :, column(me)],
            dst_ref=router.at[:, :, column(me)],
            send_sem=zero_send.at[k],
            recv_sem=zero_recv.at[k],
            **at("zero", lax.rem(me + k, n)),
        )

    fetch(gate, 0, 0).wait()
    fetch(up, 0, 1).start()
    turn(0, lambda d: send.at[0, d])

    @pl.when(me != 0)
    def _():
        pl.semaphore_wait(barrier, n - 1)
        pl.semaphore_signal(here_sem, inc=1, **at("zero", 0))

    @pl.when(me == 0)
    def _():
        pl.semaphore_wait(here_sem, n - 1)
        for k in range(1, nb):
            pl.semaphore_signal(barrier, inc=1, **at("bank", lax.rem(bank + k, nb)))

    launch(0, 0, 0)

    for copy in router_in:
        copy.wait()
    part[...] = (weight_buf[...] * gain_buf[...]).astype(part.dtype)
    router[bank, :, column(me)] = part[...]

    @pl.loop(0, bulk)
    def _(e):
        for half, source in enumerate((gate, up)):
            t = 2 * e + half
            slot = lax.rem(t, slots)

            def ready():
                fetch(source, e, half).wait()

                @pl.when(t >= slots)
                def _():
                    drain(slot)

                turn(half, lambda d: send.at[slot, d])
                launch(half, e, slot)

            if half == 0:
                pl.when(e > 0)(ready)
            else:
                ready()

            @pl.when(e + 1 < experts)
            def _():
                fetch(source, e + 1, half).start()

        @pl.when((e == min(1, bulk - 1)) & (me == 0))
        def _():
            pl.semaphore_wait(barrier, nb - 1)
            for k in range(1, n):
                pl.semaphore_signal(go_sem, inc=1, **at("zero", k))

        @pl.when(e == min(2, bulk - 1))
        def _():
            @pl.when(me != 0)
            def _():
                pl.semaphore_wait(go_sem, 1)

            for k in range(1, nb):
                bank_copy(k).start()

        @pl.when(e == min(4, bulk - 1))
        def _():
            for k in range(1, nb):
                bank_copy(k).wait()
            for k in range(1, n):
                zero_copy(k).start()

        @pl.when(e >= lag)
        def _():
            settle_both(e - lag)

    @pl.loop(bulk, experts)
    def _(e):
        for half, source in enumerate((gate, up)):
            fetch(source, e, half).wait()
            turn(half, lambda d: late.at[d, half, e - bulk])

            @pl.when(e + 1 < experts)
            def _():
                fetch(source, e + 1, half).start()

    def each_late(act):
        @pl.loop(0, experts - bulk)
        def _(e):
            for half in range(2):
                for k in range(2, n, 2):
                    act(late_copy(half, e, k))

    @pl.loop(bulk - lag, bulk - 1)
    def _(e):
        settle_both(e)

    @pl.when(odd)
    def _():
        each_late(lambda copy: copy.start())

    settle_both(bulk - 1)

    for k in range(1, n):
        zero_copy(k).wait()

    @pl.loop(max(2 * bulk - slots, 0), 2 * bulk)
    def _(t):
        drain(lax.rem(t, slots))

    @pl.when(odd)
    def _():
        each_late(lambda copy: copy.wait())


def cross(
    n, done, late, early, bulk_gate, bulk_up, final, scale_gate, scale_up,
    wide, send_sem, recv_sem, go_sem,
):
    _, _, experts, width, rows = late.shape
    me = lax.axis_index("zero")
    odd = lax.rem(me, 2) == 1
    first = bulk_gate.shape[0] - experts

    def copy(half, e, k):
        peer = lax.rem(me + k, n)
        return pltpu.make_async_remote_copy(
            src_ref=late.at[peer, half, e],
            dst_ref=final.at[me, half, e],
            send_sem=send_sem.at[2 * e + half, k],
            recv_sem=recv_sem.at[2 * e + half, k],
            **at("zero", peer),
        )

    def each(start, act):
        @pl.loop(0, experts)
        def _(e):
            for half in range(2):
                for k in range(start, n, 2):
                    act(copy(half, e, k))

    barrier = pltpu.get_barrier_semaphore()

    @pl.when(jnp.logical_not(odd))
    def _():
        for k in range(2, n, 2):
            pl.semaphore_signal(barrier, inc=1, **at("zero", lax.rem(me + k, n)))
        pl.semaphore_wait(barrier, n // 2 - 1)
        each(2, lambda c: c.start())
        for k in range(1, n, 2):
            pl.semaphore_signal(barrier, inc=1, **at("zero", lax.rem(me + k, n)))

    @pl.when(odd)
    def _():
        pl.semaphore_wait(barrier, n // 2)
        for k in range(1, n, 2):
            pl.semaphore_signal(go_sem, inc=1, **at("zero", lax.rem(me + k, n)))

    def own():
        scale_gate[...] = bulk_gate[...]
        scale_up[...] = bulk_up[...]

        @pl.loop(0, experts)
        def _(e):
            for half in range(2):
                final[me, half, e] = late[me, half, e]

    @pl.when(jnp.logical_not(odd))
    def _():
        own()
        pl.semaphore_wait(go_sem, n // 2)

    each(1, lambda c: c.start())

    @pl.when(odd)
    def _():
        own()

        @pl.loop(0, experts)
        def _(e):
            for half in range(2):
                for k in range(2, n, 2):
                    source = lax.rem(me - k + n, n)
                    final[source, half, e] = early[source // 2, half, e]

    @pl.loop(0, experts)
    def _(e):
        for half, scale in enumerate((scale_gate, scale_up)):

            def block(k):
                return final.at[lax.rem(me - k + n, n), half, e]

            def arrive(k):
                def landed():
                    pltpu.make_async_remote_copy(
                        src_ref=block(k),
                        dst_ref=block(k),
                        send_sem=send_sem.at[0, 0],
                        recv_sem=recv_sem.at[2 * e + half, k],
                        **at("zero", lax.rem(me - k + n, n)),
                    ).wait_recv()

                if k % 2:
                    landed()
                elif k:
                    pl.when(jnp.logical_not(odd))(landed)

            settle(n, block, arrive, wide, scale, first + e)

    each(1, lambda c: c.wait_send())

    @pl.when(jnp.logical_not(odd))
    def _():
        each(2, lambda c: c.wait_send())


def copy_out(source, outs, first, sem):
    n, _, count, _, rows = source.shape
    return [
        pltpu.make_async_copy(
            source.at[s, half],
            out.at[first : first + count, :, s * rows : (s + 1) * rows],
            sem.at[s, half],
        )
        for s in range(n)
        for half, out in enumerate(outs)
    ]


def run(copies):
    for copy in copies:
        copy.start()
    for copy in copies:
        copy.wait()


def finish_bulk(recv, router, ready_gate, ready_up, router_out, done, sem, router_sem):
    done[...] = jnp.zeros_like(done)
    copies = copy_out(recv, (ready_gate, ready_up), 0, sem)
    run(copies + [pltpu.make_async_copy(router, router_out, router_sem)])


def finish_rest(
    final, scale_gate, scale_up, gate_in, up_in, ready_gate, ready_up, scale_gate_out, scale_up_out, sem, scale_sem,
):
    copies = copy_out(final, (ready_gate, ready_up), ready_gate.shape[0] - final.shape[2], sem)
    copies.append(pltpu.make_async_copy(scale_gate, scale_gate_out, scale_sem.at[0]))
    copies.append(pltpu.make_async_copy(scale_up, scale_up_out, scale_sem.at[1]))
    run(copies)


def solution(mesh):
    n, nb = mesh.shape["zero"], mesh.shape["bank"]

    def local(train_gate, train_up, router_weight, router_gain):
        experts, rows, cols = train_gate.shape
        width = cols // n
        d_model = rows * n
        mine = router_weight.shape[1]
        rest = min(max(round(experts * TAIL), 1), experts - 1)
        bulk = experts - rest
        slots = min(SLOTS, 2 * bulk)
        hbm = pl.BlockSpec(memory_space=pltpu.HBM)
        inside = pl.BlockSpec(memory_space=pltpu.VMEM)
        padded = -(-width // LANES) * LANES
        scale = jax.ShapeDtypeStruct((experts, width), jnp.float32)
        joined = jax.ShapeDtypeStruct((nb, mine, d_model), jnp.bfloat16)

        def blocks(sources, count):
            return jax.ShapeDtypeStruct((sources, 2, count, width, rows), jnp.bfloat16)

        recv, router, bulk_gate, bulk_up, late, early = pl.pallas_call(
            functools.partial(exchange, n, nb),
            out_shape=(blocks(n, bulk), joined, scale, scale, blocks(n, rest), blocks(n // 2, rest)),
            in_specs=[hbm] * 4,
            out_specs=(inside,) * 6,
            scratch_shapes=[
                pltpu.VMEM((2, rows, cols), jnp.float32),
                pltpu.VMEM((cols, rows), jnp.float32),
                pltpu.VMEM((slots, n, width, rows), jnp.bfloat16),
                pltpu.VMEM((mine, rows), jnp.bfloat16),
                pltpu.VMEM((padded, LANES), jnp.float32),
                pltpu.VMEM((mine, rows), jnp.float32),
                pltpu.VMEM((1, rows), jnp.float32),
                pltpu.SemaphoreType.DMA((2,)),
                pltpu.SemaphoreType.DMA((2,)),
                pltpu.SemaphoreType.DMA((slots, n)),
                pltpu.SemaphoreType.DMA((2 * bulk, n)),
                pltpu.SemaphoreType.DMA((2 * rest, n)),
                pltpu.SemaphoreType.DMA((2 * rest, n)),
                pltpu.SemaphoreType.DMA((nb,)),
                pltpu.SemaphoreType.DMA((nb,)),
                pltpu.SemaphoreType.DMA((n,)),
                pltpu.SemaphoreType.DMA((n,)),
                pltpu.SemaphoreType.REGULAR,
                pltpu.SemaphoreType.REGULAR,
            ],
            compiler_params=pltpu.CompilerParams(
                collective_id=0, has_side_effects=True, vmem_limit_bytes=EXCHANGE_VMEM
            ),
        )(
            train_gate,
            train_up,
            pltpu.with_memory_space_constraint(router_weight.T, pltpu.HBM),
            pltpu.with_memory_space_constraint(router_gain[None, :], pltpu.HBM),
        )

        ready = jax.ShapeDtypeStruct((experts, width, d_model), jnp.bfloat16)
        ready_gate, ready_up, router, done = pl.pallas_call(
            finish_bulk,
            out_shape=(ready, ready, joined, jax.ShapeDtypeStruct((8, LANES), jnp.float32)),
            in_specs=[inside] * 2,
            out_specs=(hbm,) * 3 + (inside,),
            scratch_shapes=[pltpu.SemaphoreType.DMA((n, 2)), pltpu.SemaphoreType.DMA],
            compiler_params=pltpu.CompilerParams(vmem_limit_bytes=FINISH_VMEM),
        )(recv, router)

        final, scale_gate, scale_up = pl.pallas_call(
            functools.partial(cross, n),
            out_shape=(blocks(n, rest), scale, scale),
            in_specs=[inside] * 5,
            out_specs=(inside,) * 3,
            scratch_shapes=[
                pltpu.VMEM((padded, LANES), jnp.float32),
                pltpu.SemaphoreType.DMA((2 * rest, n)),
                pltpu.SemaphoreType.DMA((2 * rest, n)),
                pltpu.SemaphoreType.REGULAR,
            ],
            compiler_params=pltpu.CompilerParams(
                collective_id=1, has_side_effects=True, vmem_limit_bytes=CROSS_VMEM
            ),
        )(done, late, early, bulk_gate, bulk_up)

        ready_gate, ready_up, scale_gate, scale_up = pl.pallas_call(
            finish_rest,
            out_shape=(ready, ready, scale, scale),
            in_specs=[inside] * 3 + [hbm] * 2,
            out_specs=(hbm,) * 4,
            input_output_aliases={3: 0, 4: 1},
            scratch_shapes=[pltpu.SemaphoreType.DMA((n, 2)), pltpu.SemaphoreType.DMA((2,))],
            compiler_params=pltpu.CompilerParams(vmem_limit_bytes=FINISH_VMEM),
        )(final, scale_gate, scale_up, ready_gate, ready_up)
        return (
            jnp.swapaxes(ready_gate, 1, 2),
            jnp.swapaxes(ready_up, 1, 2),
            scale_gate,
            scale_up,
            router.reshape(nb * mine, d_model).T,
        )

    in_specs = (P("bank", "zero", None), P("bank", "zero", None), P("zero", "bank"), P("zero"))
    out_specs = (
        P("bank", None, "zero"),
        P("bank", None, "zero"),
        P("bank", "zero"),
        P("bank", "zero"),
        P(),
    )
    return jax.shard_map(local, mesh=mesh, in_specs=in_specs, out_specs=out_specs, check_vma=False)
```

```python
import functools

import jax
import jax.numpy as jnp
from jax import lax
from jax.experimental import pallas as pl
from jax.experimental.pallas import tpu as pltpu
from jax.sharding import PartitionSpec as P

MESH = pl.DeviceIdType.MESH
LANES = 128
SLOTS = 8
LAG = 5
TAIL = 4 / 16
EXCHANGE_VMEM = 28 * 2**20
CROSS_VMEM = 8 * 2**20
FINISH_VMEM = 2 * 2**20


def at(axis, index):
    return dict(device_id={axis: index}, device_id_type=MESH)


def spread(mean, wide, scale, row):
    width = mean.shape[0]
    wide[0:width, :] = jnp.broadcast_to(mean, (width, LANES))
    for j in range(0, width, LANES):
        stop = min(j + LANES, width)
        line = wide[j : j + LANES, :].T[0:1, 0 : stop - j]
        here = lax.broadcasted_iota(jnp.int32, (scale.shape[0], stop - j), 0) == row
        scale[:, j:stop] = jnp.where(here, line, scale[:, j:stop])


def settle(n, blocks, arrive, wide, scale, row):
    width, rows = blocks(0).shape
    total = jnp.zeros((width, LANES), jnp.float32)
    for k in range(n):
        arrive(k)
        block = blocks(k)
        for j in range(0, rows, LANES):
            total += jnp.abs(block[:, j : j + LANES].astype(jnp.float32))
    mean = jnp.sum(total, axis=1, keepdims=True) / (rows * n)
    inverse = jnp.broadcast_to(1.0 / mean, (width, LANES))
    for k in range(n):
        block = blocks(k)
        for j in range(0, rows, LANES):
            value = block[:, j : j + LANES].astype(jnp.float32) * inverse
            block[:, j : j + LANES] = value.astype(block.dtype)
    spread(mean, wide, scale, row)


def exchange(
    n, nb, gate, up, weight, gain, recv, router, scale_gate, scale_up, late, early,
    inbuf, turned, send, part, wide, weight_buf, gain_buf,
    in_sem, router_sem, send_sem, recv_sem, late_send, late_recv,
    bank_send, bank_recv, zero_send, zero_recv, here_sem, go_sem,
):
    experts, rows, cols = gate.shape
    width = cols // n
    bulk = recv.shape[2]
    slots = send.shape[0]
    lag = min(LAG, bulk)
    me = lax.axis_index("zero")
    bank = lax.axis_index("bank")
    odd = lax.rem(me, 2) == 1

    def fetch(source, e, slot):
        return pltpu.make_async_copy(source.at[e], inbuf.at[slot], in_sem.at[slot])

    router_in = (
        pltpu.make_async_copy(weight, weight_buf, router_sem.at[0]),
        pltpu.make_async_copy(gain, gain_buf, router_sem.at[1]),
    )

    fetch(gate, 0, 0).start()

    barrier = pltpu.get_barrier_semaphore()
    for k in range(1, n):
        peer = lax.rem(me + k, n)

        @pl.when(peer != 0)
        def _():
            pl.semaphore_signal(barrier, inc=1, **at("zero", peer))

    for copy in router_in:
        copy.start()
    scale_gate[...] = jnp.zeros_like(scale_gate)
    scale_up[...] = jnp.zeros_like(scale_up)

    def peer_copy(half, e, slot, k):
        peer = lax.rem(me + k, n)
        return pltpu.make_async_remote_copy(
            src_ref=send.at[slot, peer],
            dst_ref=recv.at[me, half, e],
            send_sem=send_sem.at[slot, k],
            recv_sem=recv_sem.at[2 * e + half, k],
            **at("zero", peer),
        )

    def late_copy(half, e, k):
        peer = lax.rem(me + k, n)
        return pltpu.make_async_remote_copy(
            src_ref=late.at[peer, half, e],
            dst_ref=early.at[me // 2, half, e],
            send_sem=late_send.at[2 * e + half, k],
            recv_sem=late_recv.at[2 * e + half, k],
            **at("zero", peer),
        )

    def turn(half, target):
        for j in range(0, cols, LANES):
            turned[j : j + LANES, :] = inbuf[half, :, j : j + LANES].T
        for d in range(n):
            target(d)[...] = turned[d * width : (d + 1) * width, :].astype(send.dtype)

    def drain(slot):
        for k in range(1, n):
            peer_copy(0, 0, slot, k).wait_send()

    def launch(half, e, slot):
        for k in range(1, n):
            peer_copy(half, e, slot, k).start()
        recv[me, half, e] = send[slot, me]

    def settle_both(e):
        for half, scale in enumerate((scale_gate, scale_up)):

            def block(k):
                return recv.at[lax.rem(me - k + n, n), half, e]

            def arrive(k):
                if k > 0:
                    pltpu.make_async_remote_copy(
                        src_ref=block(k),
                        dst_ref=block(k),
                        send_sem=send_sem.at[0, 0],
                        recv_sem=recv_sem.at[2 * e + half, k],
                        **at("zero", lax.rem(me - k + n, n)),
                    ).wait_recv()

            settle(n, block, arrive, wide, scale, e)

    def column(z):
        return pl.ds(pl.multiple_of(z * rows, rows), rows)

    def bank_copy(k):
        return pltpu.make_async_remote_copy(
            src_ref=part,
            dst_ref=router.at[bank, :, column(me)],
            send_sem=bank_send.at[k],
            recv_sem=bank_recv.at[k],
            **at("bank", lax.rem(bank + k, nb)),
        )

    def zero_copy(k):
        return pltpu.make_async_remote_copy(
            src_ref=router.at[:, :, column(me)],
            dst_ref=router.at[:, :, column(me)],
            send_sem=zero_send.at[k],
            recv_sem=zero_recv.at[k],
            **at("zero", lax.rem(me + k, n)),
        )

    fetch(gate, 0, 0).wait()
    fetch(up, 0, 1).start()
    turn(0, lambda d: send.at[0, d])

    @pl.when(me != 0)
    def _():
        pl.semaphore_wait(barrier, n - 1)
        pl.semaphore_signal(here_sem, inc=1, **at("zero", 0))

    @pl.when(me == 0)
    def _():
        pl.semaphore_wait(here_sem, n - 1)
        for k in range(1, nb):
            pl.semaphore_signal(barrier, inc=1, **at("bank", lax.rem(bank + k, nb)))

    launch(0, 0, 0)

    for copy in router_in:
        copy.wait()
    part[...] = (weight_buf[...] * gain_buf[...]).astype(part.dtype)
    router[bank, :, column(me)] = part[...]

    @pl.loop(0, bulk)
    def _(e):
        for half, source in enumerate((gate, up)):
            t = 2 * e + half
            slot = lax.rem(t, slots)

            def ready():
                fetch(source, e, half).wait()

                @pl.when(t >= slots)
                def _():
                    drain(slot)

                turn(half, lambda d: send.at[slot, d])
                launch(half, e, slot)

            if half == 0:
                pl.when(e > 0)(ready)
            else:
                ready()

            @pl.when(e + 1 < experts)
            def _():
                fetch(source, e + 1, half).start()

        @pl.when((e == min(1, bulk - 1)) & (me == 0))
        def _():
            pl.semaphore_wait(barrier, nb - 1)
            for k in range(1, n):
                pl.semaphore_signal(go_sem, inc=1, **at("zero", k))

        @pl.when(e == min(2, bulk - 1))
        def _():
            @pl.when(me != 0)
            def _():
                pl.semaphore_wait(go_sem, 1)

            for k in range(1, nb):
                bank_copy(k).start()

        @pl.when(e == min(4, bulk - 1))
        def _():
            for k in range(1, nb):
                bank_copy(k).wait()
            for k in range(1, n):
                zero_copy(k).start()

        @pl.when(e >= lag)
        def _():
            settle_both(e - lag)

    @pl.loop(bulk, experts)
    def _(e):
        for half, source in enumerate((gate, up)):
            fetch(source, e, half).wait()
            turn(half, lambda d: late.at[d, half, e - bulk])

            @pl.when(e + 1 < experts)
            def _():
                fetch(source, e + 1, half).start()

    def each_late(act):
        @pl.loop(0, experts - bulk)
        def _(e):
            for half in range(2):
                for k in range(2, n, 2):
                    act(late_copy(half, e, k))

    @pl.loop(bulk - lag, bulk - 1)
    def _(e):
        settle_both(e)

    @pl.when(odd)
    def _():
        each_late(lambda copy: copy.start())

    settle_both(bulk - 1)

    for k in range(1, n):
        zero_copy(k).wait()

    @pl.loop(max(2 * bulk - slots, 0), 2 * bulk)
    def _(t):
        drain(lax.rem(t, slots))

    @pl.when(odd)
    def _():
        each_late(lambda copy: copy.wait())


def cross(
    n, done, late, early, bulk_gate, bulk_up, final, scale_gate, scale_up,
    wide, send_sem, recv_sem, go_sem,
):
    _, _, experts, width, rows = late.shape
    me = lax.axis_index("zero")
    odd = lax.rem(me, 2) == 1
    first = bulk_gate.shape[0] - experts

    def copy(half, e, k):
        peer = lax.rem(me + k, n)
        return pltpu.make_async_remote_copy(
            src_ref=late.at[peer, half, e],
            dst_ref=final.at[me, half, e],
            send_sem=send_sem.at[2 * e + half, k],
            recv_sem=recv_sem.at[2 * e + half, k],
            **at("zero", peer),
        )

    def each(start, act):
        @pl.loop(0, experts)
        def _(e):
            for half in range(2):
                for k in range(start, n, 2):
                    act(copy(half, e, k))

    barrier = pltpu.get_barrier_semaphore()

    @pl.when(jnp.logical_not(odd))
    def _():
        for k in range(2, n, 2):
            pl.semaphore_signal(barrier, inc=1, **at("zero", lax.rem(me + k, n)))
        pl.semaphore_wait(barrier, n // 2 - 1)
        each(2, lambda c: c.start())
        for k in range(1, n, 2):
            pl.semaphore_signal(barrier, inc=1, **at("zero", lax.rem(me + k, n)))

    @pl.when(odd)
    def _():
        pl.semaphore_wait(barrier, n // 2)
        for k in range(1, n, 2):
            pl.semaphore_signal(go_sem, inc=1, **at("zero", lax.rem(me + k, n)))

    def own():
        scale_gate[...] = bulk_gate[...]
        scale_up[...] = bulk_up[...]

        @pl.loop(0, experts)
        def _(e):
            for half in range(2):
                final[me, half, e] = late[me, half, e]

    @pl.when(jnp.logical_not(odd))
    def _():
        own()
        pl.semaphore_wait(go_sem, n // 2)

    each(1, lambda c: c.start())

    @pl.when(odd)
    def _():
        own()

        @pl.loop(0, experts)
        def _(e):
            for half in range(2):
                for k in range(2, n, 2):
                    source = lax.rem(me - k + n, n)
                    final[source, half, e] = early[source // 2, half, e]

    @pl.loop(0, experts)
    def _(e):
        for half, scale in enumerate((scale_gate, scale_up)):

            def block(k):
                return final.at[lax.rem(me - k + n, n), half, e]

            def arrive(k):
                def landed():
                    pltpu.make_async_remote_copy(
                        src_ref=block(k),
                        dst_ref=block(k),
                        send_sem=send_sem.at[0, 0],
                        recv_sem=recv_sem.at[2 * e + half, k],
                        **at("zero", lax.rem(me - k + n, n)),
                    ).wait_recv()

                if k % 2:
                    landed()
                elif k:
                    pl.when(jnp.logical_not(odd))(landed)

            settle(n, block, arrive, wide, scale, first + e)

    each(1, lambda c: c.wait_send())

    @pl.when(jnp.logical_not(odd))
    def _():
        each(2, lambda c: c.wait_send())


def copy_out(source, outs, first, sem):
    n, _, count, _, rows = source.shape
    return [
        pltpu.make_async_copy(
            source.at[s, half],
            out.at[first : first + count, :, s * rows : (s + 1) * rows],
            sem.at[s, half],
        )
        for s in range(n)
        for half, out in enumerate(outs)
    ]


def run(copies):
    for copy in copies:
        copy.start()
    for copy in copies:
        copy.wait()


def finish_bulk(recv, router, ready_gate, ready_up, router_out, done, sem, router_sem):
    done[...] = jnp.zeros_like(done)
    copies = copy_out(recv, (ready_gate, ready_up), 0, sem)
    run(copies + [pltpu.make_async_copy(router, router_out, router_sem)])


def finish_rest(
    final, scale_gate, scale_up, gate_in, up_in, ready_gate, ready_up, scale_gate_out, scale_up_out, sem, scale_sem,
):
    copies = copy_out(final, (ready_gate, ready_up), ready_gate.shape[0] - final.shape[2], sem)
    copies.append(pltpu.make_async_copy(scale_gate, scale_gate_out, scale_sem.at[0]))
    copies.append(pltpu.make_async_copy(scale_up, scale_up_out, scale_sem.at[1]))
    run(copies)


def solution(mesh):
    n, nb = mesh.shape["zero"], mesh.shape["bank"]

    def local(train_gate, train_up, router_weight, router_gain):
        experts, rows, cols = train_gate.shape
        width = cols // n
        d_model = rows * n
        mine = router_weight.shape[1]
        rest = min(max(round(experts * TAIL), 1), experts - 1)
        bulk = experts - rest
        slots = min(SLOTS, 2 * bulk)
        hbm = pl.BlockSpec(memory_space=pltpu.HBM)
        inside = pl.BlockSpec(memory_space=pltpu.VMEM)
        padded = -(-width // LANES) * LANES
        scale = jax.ShapeDtypeStruct((experts, width), jnp.float32)
        joined = jax.ShapeDtypeStruct((nb, mine, d_model), jnp.bfloat16)

        def blocks(sources, count):
            return jax.ShapeDtypeStruct((sources, 2, count, width, rows), jnp.bfloat16)

        recv, router, bulk_gate, bulk_up, late, early = pl.pallas_call(
            functools.partial(exchange, n, nb),
            out_shape=(blocks(n, bulk), joined, scale, scale, blocks(n, rest), blocks(n // 2, rest)),
            in_specs=[hbm] * 4,
            out_specs=(inside,) * 6,
            scratch_shapes=[
                pltpu.VMEM((2, rows, cols), jnp.float32),
                pltpu.VMEM((cols, rows), jnp.float32),
                pltpu.VMEM((slots, n, width, rows), jnp.bfloat16),
                pltpu.VMEM((mine, rows), jnp.bfloat16),
                pltpu.VMEM((padded, LANES), jnp.float32),
                pltpu.VMEM((mine, rows), jnp.float32),
                pltpu.VMEM((1, rows), jnp.float32),
                pltpu.SemaphoreType.DMA((2,)),
                pltpu.SemaphoreType.DMA((2,)),
                pltpu.SemaphoreType.DMA((slots, n)),
                pltpu.SemaphoreType.DMA((2 * bulk, n)),
                pltpu.SemaphoreType.DMA((2 * rest, n)),
                pltpu.SemaphoreType.DMA((2 * rest, n)),
                pltpu.SemaphoreType.DMA((nb,)),
                pltpu.SemaphoreType.DMA((nb,)),
                pltpu.SemaphoreType.DMA((n,)),
                pltpu.SemaphoreType.DMA((n,)),
                pltpu.SemaphoreType.REGULAR,
                pltpu.SemaphoreType.REGULAR,
            ],
            compiler_params=pltpu.CompilerParams(
                collective_id=0, has_side_effects=True, vmem_limit_bytes=EXCHANGE_VMEM
            ),
        )(
            train_gate,
            train_up,
            pltpu.with_memory_space_constraint(router_weight.T, pltpu.HBM),
            pltpu.with_memory_space_constraint(router_gain[None, :], pltpu.HBM),
        )

        ready = jax.ShapeDtypeStruct((experts, width, d_model), jnp.bfloat16)
        ready_gate, ready_up, router, done = pl.pallas_call(
            finish_bulk,
            out_shape=(ready, ready, joined, jax.ShapeDtypeStruct((8, LANES), jnp.float32)),
            in_specs=[inside] * 2,
            out_specs=(hbm,) * 3 + (inside,),
            scratch_shapes=[pltpu.SemaphoreType.DMA((n, 2)), pltpu.SemaphoreType.DMA],
            compiler_params=pltpu.CompilerParams(vmem_limit_bytes=FINISH_VMEM),
        )(recv, router)

        final, scale_gate, scale_up = pl.pallas_call(
            functools.partial(cross, n),
            out_shape=(blocks(n, rest), scale, scale),
            in_specs=[inside] * 5,
            out_specs=(inside,) * 3,
            scratch_shapes=[
                pltpu.VMEM((padded, LANES), jnp.float32),
                pltpu.SemaphoreType.DMA((2 * rest, n)),
                pltpu.SemaphoreType.DMA((2 * rest, n)),
                pltpu.SemaphoreType.REGULAR,
            ],
            compiler_params=pltpu.CompilerParams(
                collective_id=1, has_side_effects=True, vmem_limit_bytes=CROSS_VMEM
            ),
        )(done, late, early, bulk_gate, bulk_up)

        ready_gate, ready_up, scale_gate, scale_up = pl.pallas_call(
            finish_rest,
            out_shape=(ready, ready, scale, scale),
            in_specs=[inside] * 3 + [hbm] * 2,
            out_specs=(hbm,) * 4,
            input_output_aliases={3: 0, 4: 1},
            scratch_shapes=[pltpu.SemaphoreType.DMA((n, 2)), pltpu.SemaphoreType.DMA((2,))],
            compiler_params=pltpu.CompilerParams(vmem_limit_bytes=FINISH_VMEM),
        )(final, scale_gate, scale_up, ready_gate, ready_up)
        return (
            jnp.swapaxes(ready_gate, 1, 2),
            jnp.swapaxes(ready_up, 1, 2),
            scale_gate,
            scale_up,
            router.reshape(nb * mine, d_model).T,
        )

    in_specs = (P("bank", "zero", None), P("bank", "zero", None), P("zero", "bank"), P("zero"))
    out_specs = (
        P("bank", None, "zero"),
        P("bank", None, "zero"),
        P("bank", "zero"),
        P("bank", "zero"),
        P(),
    )
    return jax.shard_map(local, mesh=mesh, in_specs=in_specs, out_specs=out_specs, check_vma=False)
```

```python
import functools

import jax
import jax.numpy as jnp
from jax import lax
from jax.experimental import pallas as pl
from jax.experimental.pallas import tpu as pltpu
from jax.sharding import PartitionSpec as P

MESH = pl.DeviceIdType.MESH
LANES = 128
SLOTS = 4
LAG = 5
TAIL = 4 / 16
EXCHANGE_VMEM = 28 * 2**20
CROSS_VMEM = 8 * 2**20
FINISH_VMEM = 2 * 2**20


def at(axis, index):
    return dict(device_id={axis: index}, device_id_type=MESH)


def spread(mean, wide, scale, row):
    width = mean.shape[0]
    wide[0:width, :] = jnp.broadcast_to(mean, (width, LANES))
    for j in range(0, width, LANES):
        stop = min(j + LANES, width)
        line = wide[j : j + LANES, :].T[0:1, 0 : stop - j]
        here = lax.broadcasted_iota(jnp.int32, (scale.shape[0], stop - j), 0) == row
        scale[:, j:stop] = jnp.where(here, line, scale[:, j:stop])


def settle(n, blocks, arrive, wide, scale, row):
    width, rows = blocks(0).shape
    total = jnp.zeros((width, LANES), jnp.float32)
    for k in range(n):
        arrive(k)
        block = blocks(k)
        for j in range(0, rows, LANES):
            total += jnp.abs(block[:, j : j + LANES].astype(jnp.float32))
    mean = jnp.sum(total, axis=1, keepdims=True) / (rows * n)
    inverse = jnp.broadcast_to(1.0 / mean, (width, LANES))
    for k in range(n):
        block = blocks(k)
        for j in range(0, rows, LANES):
            value = block[:, j : j + LANES].astype(jnp.float32) * inverse
            block[:, j : j + LANES] = value.astype(block.dtype)
    spread(mean, wide, scale, row)


def exchange(
    n, nb, gate, up, weight, gain, recv, router, scale_gate, scale_up, late, early,
    inbuf, turned, send, part, wide, weight_buf, gain_buf,
    in_sem, router_sem, send_sem, recv_sem, late_send, late_recv,
    bank_send, bank_recv, zero_send, zero_recv, here_sem, go_sem,
):
    experts, rows, cols = gate.shape
    width = cols // n
    bulk = recv.shape[1]
    slots = send.shape[0]
    lag = min(LAG, bulk)
    me = lax.axis_index("zero")
    bank = lax.axis_index("bank")
    odd = lax.rem(me, 2) == 1

    def fetch(source, e, slot):
        return pltpu.make_async_copy(source.at[e], inbuf.at[slot], in_sem.at[slot])

    router_in = (
        pltpu.make_async_copy(weight, weight_buf, router_sem.at[0]),
        pltpu.make_async_copy(gain, gain_buf, router_sem.at[1]),
    )

    fetch(gate, 0, 0).start()

    barrier = pltpu.get_barrier_semaphore()
    for k in range(1, n):
        peer = lax.rem(me + k, n)

        @pl.when(peer != 0)
        def _():
            pl.semaphore_signal(barrier, inc=1, **at("zero", peer))

    for copy in router_in:
        copy.start()
    scale_gate[...] = jnp.zeros_like(scale_gate)
    scale_up[...] = jnp.zeros_like(scale_up)

    def peer_copy(e, slot, k, part_of=lambda ref: ref):
        peer = lax.rem(me + k, n)
        return pltpu.make_async_remote_copy(
            src_ref=part_of(send.at[slot, peer]),
            dst_ref=part_of(recv.at[me, e]),
            send_sem=send_sem.at[slot, k],
            recv_sem=recv_sem.at[e, k],
            **at("zero", peer),
        )

    def late_copy(e, k):
        peer = lax.rem(me + k, n)
        return pltpu.make_async_remote_copy(
            src_ref=late.at[peer, e],
            dst_ref=early.at[me // 2, e],
            send_sem=late_send.at[e, k],
            recv_sem=late_recv.at[e, k],
            **at("zero", peer),
        )

    def turn(half, target):
        for j in range(0, cols, LANES):
            turned[j : j + LANES, :] = inbuf[half, :, j : j + LANES].T
        for d in range(n):
            target(d)[...] = turned[d * width : (d + 1) * width, :].astype(send.dtype)

    def drain(slot):
        for k in range(1, n):
            peer_copy(0, slot, k).wait_send()

    def launch(e, slot, half=None):
        def part_of(ref):
            return ref if half is None else ref.at[half]

        for k in range(1, n):
            peer_copy(e, slot, k, part_of).start()
        part_of(recv.at[me, e])[...] = part_of(send.at[slot, me])[...]

    def settle_both(e):
        for half, scale in enumerate((scale_gate, scale_up)):

            def block(k):
                return recv.at[lax.rem(me - k + n, n), e, half]

            def arrive(k):
                if k > 0 and half == 0:
                    source = lax.rem(me - k + n, n)
                    pltpu.make_async_remote_copy(
                        src_ref=recv.at[source, e],
                        dst_ref=recv.at[source, e],
                        send_sem=send_sem.at[0, 0],
                        recv_sem=recv_sem.at[e, k],
                        **at("zero", source),
                    ).wait_recv()

            settle(n, block, arrive, wide, scale, e)

    def column(z):
        return pl.ds(pl.multiple_of(z * rows, rows), rows)

    def bank_copy(k):
        return pltpu.make_async_remote_copy(
            src_ref=part,
            dst_ref=router.at[bank, :, column(me)],
            send_sem=bank_send.at[k],
            recv_sem=bank_recv.at[k],
            **at("bank", lax.rem(bank + k, nb)),
        )

    def zero_copy(k):
        return pltpu.make_async_remote_copy(
            src_ref=router.at[:, :, column(me)],
            dst_ref=router.at[:, :, column(me)],
            send_sem=zero_send.at[k],
            recv_sem=zero_recv.at[k],
            **at("zero", lax.rem(me + k, n)),
        )

    fetch(gate, 0, 0).wait()
    fetch(up, 0, 1).start()
    turn(0, lambda d: send.at[0, d, 0])
    fetch(gate, 1, 0).start()

    @pl.when(me != 0)
    def _():
        pl.semaphore_wait(barrier, n - 1)
        pl.semaphore_signal(here_sem, inc=1, **at("zero", 0))

    @pl.when(me == 0)
    def _():
        pl.semaphore_wait(here_sem, n - 1)
        for k in range(1, nb):
            pl.semaphore_signal(barrier, inc=1, **at("bank", lax.rem(bank + k, nb)))

    launch(0, 0, 0)

    fetch(up, 0, 1).wait()
    turn(1, lambda d: send.at[0, d, 1])
    fetch(up, 1, 1).start()
    launch(0, 0, 1)

    for copy in router_in:
        copy.wait()
    part[...] = (weight_buf[...] * gain_buf[...]).astype(part.dtype)
    router[bank, :, column(me)] = part[...]

    @pl.loop(1, bulk)
    def _(e):
        slot = lax.rem(e, slots)

        @pl.when(e >= slots)
        def _():
            drain(slot)

        for half, source in enumerate((gate, up)):
            fetch(source, e, half).wait()
            turn(half, lambda d: send.at[slot, d, half])

            @pl.when(e + 1 < experts)
            def _():
                fetch(source, e + 1, half).start()

        launch(e, slot)

        @pl.when((e == min(1, bulk - 1)) & (me == 0))
        def _():
            pl.semaphore_wait(barrier, nb - 1)
            for k in range(1, n):
                pl.semaphore_signal(go_sem, inc=1, **at("zero", k))

        @pl.when(e == min(2, bulk - 1))
        def _():
            @pl.when(me != 0)
            def _():
                pl.semaphore_wait(go_sem, 1)

            for k in range(1, nb):
                bank_copy(k).start()

        @pl.when(e == min(4, bulk - 1))
        def _():
            for k in range(1, nb):
                bank_copy(k).wait()
            for k in range(1, n):
                zero_copy(k).start()

        @pl.when(e >= lag)
        def _():
            settle_both(e - lag)

    @pl.loop(bulk, experts)
    def _(e):
        for half, source in enumerate((gate, up)):
            fetch(source, e, half).wait()
            turn(half, lambda d: late.at[d, e - bulk, half])

            @pl.when(e + 1 < experts)
            def _():
                fetch(source, e + 1, half).start()

    def each_late(act):
        @pl.loop(0, experts - bulk)
        def _(e):
            for k in range(2, n, 2):
                act(late_copy(e, k))

    @pl.loop(bulk - lag, bulk - 1)
    def _(e):
        settle_both(e)

    @pl.when(odd)
    def _():
        each_late(lambda copy: copy.start())

    settle_both(bulk - 1)

    for k in range(1, n):
        zero_copy(k).wait()

    @pl.loop(bulk - slots, bulk)
    def _(e):
        drain(lax.rem(e, slots))

    @pl.when(odd)
    def _():
        each_late(lambda copy: copy.wait())


def cross(
    n, done, late, early, bulk_gate, bulk_up, final, scale_gate, scale_up,
    wide, send_sem, recv_sem, go_sem,
):
    experts = late.shape[1]
    me = lax.axis_index("zero")
    odd = lax.rem(me, 2) == 1
    first = bulk_gate.shape[0] - experts

    last = experts - 1

    def copy(e, k, half=None):
        peer = lax.rem(me + k, n)
        row = e if half is None else e + half

        def part_of(ref):
            return ref if half is None else ref.at[half]

        return pltpu.make_async_remote_copy(
            src_ref=part_of(late.at[peer, e]),
            dst_ref=part_of(final.at[me, e]),
            send_sem=send_sem.at[row, k],
            recv_sem=recv_sem.at[row, k],
            **at("zero", peer),
        )

    def each(start, act):
        @pl.loop(0, last)
        def _(e):
            for k in range(start, n, 2):
                act(copy(e, k))

        for half in range(2):
            for k in range(start, n, 2):
                act(copy(last, k, half))

    def step(e, halves):
        for half, scale in enumerate((scale_gate, scale_up)):

            def block(k):
                return final.at[lax.rem(me - k + n, n), e, half]

            def arrive(k):
                source = lax.rem(me - k + n, n)
                arrived = block(k) if halves else final.at[source, e]

                def landed():
                    pltpu.make_async_remote_copy(
                        src_ref=arrived,
                        dst_ref=arrived,
                        send_sem=send_sem.at[0, 0],
                        recv_sem=recv_sem.at[e + half, k],
                        **at("zero", source),
                    ).wait_recv()

                if halves or half == 0:
                    if k % 2:
                        landed()
                    elif k:
                        pl.when(jnp.logical_not(odd))(landed)

            settle(n, block, arrive, wide, scale, first + e)

    barrier = pltpu.get_barrier_semaphore()

    @pl.when(jnp.logical_not(odd))
    def _():
        for k in range(2, n, 2):
            pl.semaphore_signal(barrier, inc=1, **at("zero", lax.rem(me + k, n)))
        pl.semaphore_wait(barrier, n // 2 - 1)
        each(2, lambda c: c.start())
        for k in range(1, n, 2):
            pl.semaphore_signal(barrier, inc=1, **at("zero", lax.rem(me + k, n)))

    @pl.when(odd)
    def _():
        pl.semaphore_wait(barrier, n // 2)
        for k in range(1, n, 2):
            pl.semaphore_signal(go_sem, inc=1, **at("zero", lax.rem(me + k, n)))

    def own():
        scale_gate[...] = bulk_gate[...]
        scale_up[...] = bulk_up[...]

        @pl.loop(0, experts)
        def _(e):
            final[me, e] = late[me, e]

    @pl.when(jnp.logical_not(odd))
    def _():
        own()
        pl.semaphore_wait(go_sem, n // 2)

    @pl.when(odd)
    def _():
        own()

        @pl.loop(0, experts)
        def _(e):
            for k in range(2, n, 2):
                source = lax.rem(me - k + n, n)
                final[source, e] = early[source // 2, e]

    each(1, lambda c: c.start())

    @pl.loop(0, last)
    def _(e):
        step(e, False)

    step(last, True)

    each(1, lambda c: c.wait_send())

    @pl.when(jnp.logical_not(odd))
    def _():
        each(2, lambda c: c.wait_send())


def copy_out(source, outs, first, sem):
    n, count, _, _, rows = source.shape
    return [
        pltpu.make_async_copy(
            source.at[s, :, half],
            out.at[first : first + count, :, s * rows : (s + 1) * rows],
            sem.at[s, half],
        )
        for s in range(n)
        for half, out in enumerate(outs)
    ]


def run(copies):
    for copy in copies:
        copy.start()
    for copy in copies:
        copy.wait()


def finish_bulk(recv, router, ready_gate, ready_up, router_out, done, sem, router_sem):
    done[...] = jnp.zeros_like(done)
    copies = copy_out(recv, (ready_gate, ready_up), 0, sem)
    run(copies + [pltpu.make_async_copy(router, router_out, router_sem)])


def finish_rest(
    final, scale_gate, scale_up, gate_in, up_in, ready_gate, ready_up, scale_gate_out, scale_up_out, sem, scale_sem,
):
    copies = copy_out(final, (ready_gate, ready_up), ready_gate.shape[0] - final.shape[1], sem)
    copies.append(pltpu.make_async_copy(scale_gate, scale_gate_out, scale_sem.at[0]))
    copies.append(pltpu.make_async_copy(scale_up, scale_up_out, scale_sem.at[1]))
    run(copies)


def solution(mesh):
    n, nb = mesh.shape["zero"], mesh.shape["bank"]

    def local(train_gate, train_up, router_weight, router_gain):
        experts, rows, cols = train_gate.shape
        width = cols // n
        d_model = rows * n
        mine = router_weight.shape[1]
        rest = min(max(round(experts * TAIL), 1), experts - 1)
        bulk = experts - rest
        slots = min(SLOTS, bulk)
        hbm = pl.BlockSpec(memory_space=pltpu.HBM)
        inside = pl.BlockSpec(memory_space=pltpu.VMEM)
        padded = -(-width // LANES) * LANES
        scale = jax.ShapeDtypeStruct((experts, width), jnp.float32)
        joined = jax.ShapeDtypeStruct((nb, mine, d_model), jnp.bfloat16)

        def blocks(sources, count):
            return jax.ShapeDtypeStruct((sources, count, 2, width, rows), jnp.bfloat16)

        recv, router, bulk_gate, bulk_up, late, early = pl.pallas_call(
            functools.partial(exchange, n, nb),
            out_shape=(blocks(n, bulk), joined, scale, scale, blocks(n, rest), blocks(n // 2, rest)),
            in_specs=[hbm] * 4,
            out_specs=(inside,) * 6,
            scratch_shapes=[
                pltpu.VMEM((2, rows, cols), jnp.float32),
                pltpu.VMEM((cols, rows), jnp.float32),
                pltpu.VMEM((slots, n, 2, width, rows), jnp.bfloat16),
                pltpu.VMEM((mine, rows), jnp.bfloat16),
                pltpu.VMEM((padded, LANES), jnp.float32),
                pltpu.VMEM((mine, rows), jnp.float32),
                pltpu.VMEM((1, rows), jnp.float32),
                pltpu.SemaphoreType.DMA((2,)),
                pltpu.SemaphoreType.DMA((2,)),
                pltpu.SemaphoreType.DMA((slots, n)),
                pltpu.SemaphoreType.DMA((bulk, n)),
                pltpu.SemaphoreType.DMA((rest, n)),
                pltpu.SemaphoreType.DMA((rest, n)),
                pltpu.SemaphoreType.DMA((nb,)),
                pltpu.SemaphoreType.DMA((nb,)),
                pltpu.SemaphoreType.DMA((n,)),
                pltpu.SemaphoreType.DMA((n,)),
                pltpu.SemaphoreType.REGULAR,
                pltpu.SemaphoreType.REGULAR,
            ],
            compiler_params=pltpu.CompilerParams(
                collective_id=0, has_side_effects=True, vmem_limit_bytes=EXCHANGE_VMEM
            ),
        )(
            train_gate,
            train_up,
            pltpu.with_memory_space_constraint(router_weight.T, pltpu.HBM),
            pltpu.with_memory_space_constraint(router_gain[None, :], pltpu.HBM),
        )

        ready = jax.ShapeDtypeStruct((experts, width, d_model), jnp.bfloat16)
        ready_gate, ready_up, router, done = pl.pallas_call(
            finish_bulk,
            out_shape=(ready, ready, joined, jax.ShapeDtypeStruct((8, LANES), jnp.float32)),
            in_specs=[inside] * 2,
            out_specs=(hbm,) * 3 + (inside,),
            scratch_shapes=[pltpu.SemaphoreType.DMA((n, 2)), pltpu.SemaphoreType.DMA],
            compiler_params=pltpu.CompilerParams(vmem_limit_bytes=FINISH_VMEM),
        )(recv, router)

        final, scale_gate, scale_up = pl.pallas_call(
            functools.partial(cross, n),
            out_shape=(blocks(n, rest), scale, scale),
            in_specs=[inside] * 5,
            out_specs=(inside,) * 3,
            scratch_shapes=[
                pltpu.VMEM((padded, LANES), jnp.float32),
                pltpu.SemaphoreType.DMA((rest + 1, n)),
                pltpu.SemaphoreType.DMA((rest + 1, n)),
                pltpu.SemaphoreType.REGULAR,
            ],
            compiler_params=pltpu.CompilerParams(
                collective_id=1, has_side_effects=True, vmem_limit_bytes=CROSS_VMEM
            ),
        )(done, late, early, bulk_gate, bulk_up)

        ready_gate, ready_up, scale_gate, scale_up = pl.pallas_call(
            finish_rest,
            out_shape=(ready, ready, scale, scale),
            in_specs=[inside] * 3 + [hbm] * 2,
            out_specs=(hbm,) * 4,
            input_output_aliases={3: 0, 4: 1},
            scratch_shapes=[pltpu.SemaphoreType.DMA((n, 2)), pltpu.SemaphoreType.DMA((2,))],
            compiler_params=pltpu.CompilerParams(vmem_limit_bytes=FINISH_VMEM),
        )(final, scale_gate, scale_up, ready_gate, ready_up)
        return (
            jnp.swapaxes(ready_gate, 1, 2),
            jnp.swapaxes(ready_up, 1, 2),
            scale_gate,
            scale_up,
            router.reshape(nb * mine, d_model).T,
        )

    in_specs = (P("bank", "zero", None), P("bank", "zero", None), P("zero", "bank"), P("zero"))
    out_specs = (
        P("bank", None, "zero"),
        P("bank", None, "zero"),
        P("bank", "zero"),
        P("bank", "zero"),
        P(),
    )
    return jax.shard_map(local, mesh=mesh, in_specs=in_specs, out_specs=out_specs, check_vma=False)
```

```python
import functools

import jax
import jax.numpy as jnp
from jax import lax
from jax.experimental import pallas as pl
from jax.experimental.pallas import tpu as pltpu
from jax.sharding import PartitionSpec as P

MESH = pl.DeviceIdType.MESH
LANES = 128
SLOTS = 4
LAG = 5
TAIL = 4 / 16
EXCHANGE_VMEM = 28 * 2**20
CROSS_VMEM = 8 * 2**20
FINISH_VMEM = 2 * 2**20


def at(axis, index):
    return dict(device_id={axis: index}, device_id_type=MESH)


def spread(mean, wide, scale, row):
    width = mean.shape[0]
    wide[0:width, :] = jnp.broadcast_to(mean, (width, LANES))
    for j in range(0, width, LANES):
        stop = min(j + LANES, width)
        line = wide[j : j + LANES, :].T[0:1, 0 : stop - j]
        here = lax.broadcasted_iota(jnp.int32, (scale.shape[0], stop - j), 0) == row
        scale[:, j:stop] = jnp.where(here, line, scale[:, j:stop])


def settle(n, blocks, arrive, wide, scale, row):
    width, rows = blocks(0).shape
    total = jnp.zeros((width, LANES), jnp.float32)
    for k in range(n):
        arrive(k)
        block = blocks(k)
        for j in range(0, rows, LANES):
            total += jnp.abs(block[:, j : j + LANES].astype(jnp.float32))
    mean = jnp.sum(total, axis=1, keepdims=True) / (rows * n)
    inverse = jnp.broadcast_to(1.0 / mean, (width, LANES))
    for k in range(n):
        block = blocks(k)
        for j in range(0, rows, LANES):
            value = block[:, j : j + LANES].astype(jnp.float32) * inverse
            block[:, j : j + LANES] = value.astype(block.dtype)
    spread(mean, wide, scale, row)


def exchange(
    n, nb, gate, up, weight, gain, recv, router, scale_gate, scale_up, late, early,
    inbuf, turned, send, part, wide, weight_buf, gain_buf,
    in_sem, router_sem, send_sem, recv_sem, late_send, late_recv,
    bank_send, bank_recv, zero_send, zero_recv, here_sem, go_sem,
):
    experts, rows, cols = gate.shape
    width = cols // n
    bulk = recv.shape[1]
    slots = send.shape[0]
    lag = min(LAG, bulk)
    me = lax.axis_index("zero")
    bank = lax.axis_index("bank")
    odd = lax.rem(me, 2) == 1

    def fetch(source, e, slot):
        return pltpu.make_async_copy(source.at[e], inbuf.at[slot], in_sem.at[slot])

    router_in = (
        pltpu.make_async_copy(weight, weight_buf, router_sem.at[0]),
        pltpu.make_async_copy(gain, gain_buf, router_sem.at[1]),
    )

    fetch(gate, 0, 0).start()

    barrier = pltpu.get_barrier_semaphore()
    for k in range(1, n):
        peer = lax.rem(me + k, n)

        @pl.when(peer != 0)
        def _():
            pl.semaphore_signal(barrier, inc=1, **at("zero", peer))

    for copy in router_in:
        copy.start()
    scale_gate[...] = jnp.zeros_like(scale_gate)
    scale_up[...] = jnp.zeros_like(scale_up)

    def peer_copy(e, slot, k, part_of=lambda ref: ref):
        peer = lax.rem(me + k, n)
        return pltpu.make_async_remote_copy(
            src_ref=part_of(send.at[slot, peer]),
            dst_ref=part_of(recv.at[me, e]),
            send_sem=send_sem.at[slot, k],
            recv_sem=recv_sem.at[e, k],
            **at("zero", peer),
        )

    def late_copy(e, k):
        peer = lax.rem(me + k, n)
        return pltpu.make_async_remote_copy(
            src_ref=late.at[peer, e],
            dst_ref=early.at[me // 2, e],
            send_sem=late_send.at[e, k],
            recv_sem=late_recv.at[e, k],
            **at("zero", peer),
        )

    def turn(half, target):
        for j in range(0, cols, LANES):
            turned[j : j + LANES, :] = inbuf[half, :, j : j + LANES].T
        for d in range(n):
            target(d)[...] = turned[d * width : (d + 1) * width, :].astype(send.dtype)

    def drain(slot):
        for k in range(1, n):
            peer_copy(0, slot, k).wait_send()

    def launch(e, slot, half=None):
        def part_of(ref):
            return ref if half is None else ref.at[half]

        for k in range(1, n):
            peer_copy(e, slot, k, part_of).start()
        part_of(recv.at[me, e])[...] = part_of(send.at[slot, me])[...]

    def settle_both(e):
        for half, scale in enumerate((scale_gate, scale_up)):

            def block(k):
                return recv.at[lax.rem(me - k + n, n), e, half]

            def arrive(k):
                if k > 0 and half == 0:
                    source = lax.rem(me - k + n, n)
                    pltpu.make_async_remote_copy(
                        src_ref=recv.at[source, e],
                        dst_ref=recv.at[source, e],
                        send_sem=send_sem.at[0, 0],
                        recv_sem=recv_sem.at[e, k],
                        **at("zero", source),
                    ).wait_recv()

            settle(n, block, arrive, wide, scale, e)

    def column(z):
        return pl.ds(pl.multiple_of(z * rows, rows), rows)

    def bank_copy(k):
        return pltpu.make_async_remote_copy(
            src_ref=part,
            dst_ref=router.at[bank, :, column(me)],
            send_sem=bank_send.at[k],
            recv_sem=bank_recv.at[k],
            **at("bank", lax.rem(bank + k, nb)),
        )

    def zero_copy(k):
        return pltpu.make_async_remote_copy(
            src_ref=router.at[:, :, column(me)],
            dst_ref=router.at[:, :, column(me)],
            send_sem=zero_send.at[k],
            recv_sem=zero_recv.at[k],
            **at("zero", lax.rem(me + k, n)),
        )

    fetch(gate, 0, 0).wait()
    fetch(up, 0, 1).start()
    turn(0, lambda d: send.at[0, d, 0])
    fetch(gate, 1, 0).start()

    @pl.when(me != 0)
    def _():
        pl.semaphore_wait(barrier, n - 1)
        pl.semaphore_signal(here_sem, inc=1, **at("zero", 0))

    @pl.when(me == 0)
    def _():
        pl.semaphore_wait(here_sem, n - 1)
        for k in range(1, nb):
            pl.semaphore_signal(barrier, inc=1, **at("bank", lax.rem(bank + k, nb)))

    launch(0, 0, 0)

    fetch(up, 0, 1).wait()
    turn(1, lambda d: send.at[0, d, 1])
    fetch(up, 1, 1).start()
    launch(0, 0, 1)

    for copy in router_in:
        copy.wait()
    part[...] = (weight_buf[...] * gain_buf[...]).astype(part.dtype)
    router[bank, :, column(me)] = part[...]

    @pl.loop(1, bulk)
    def _(e):
        slot = lax.rem(e, slots)

        @pl.when(e >= slots)
        def _():
            drain(slot)

        for half, source in enumerate((gate, up)):
            fetch(source, e, half).wait()
            turn(half, lambda d: send.at[slot, d, half])

            @pl.when(e + 1 < experts)
            def _():
                fetch(source, e + 1, half).start()

        launch(e, slot)

        @pl.when((e == min(1, bulk - 1)) & (me == 0))
        def _():
            pl.semaphore_wait(barrier, nb - 1)
            for k in range(1, n):
                pl.semaphore_signal(go_sem, inc=1, **at("zero", k))

        @pl.when(e == min(2, bulk - 1))
        def _():
            @pl.when(me != 0)
            def _():
                pl.semaphore_wait(go_sem, 1)

            for k in range(1, nb):
                bank_copy(k).start()

        @pl.when(e == min(4, bulk - 1))
        def _():
            for k in range(1, nb):
                bank_copy(k).wait()
            for k in range(1, n):
                zero_copy(k).start()

        @pl.when(e >= lag)
        def _():
            settle_both(e - lag)

    @pl.loop(bulk, experts)
    def _(e):
        for half, source in enumerate((gate, up)):
            fetch(source, e, half).wait()
            turn(half, lambda d: late.at[d, e - bulk, half])

            @pl.when(e + 1 < experts)
            def _():
                fetch(source, e + 1, half).start()

    def each_late(act):
        @pl.loop(0, experts - bulk)
        def _(e):
            for k in range(2, n, 2):
                act(late_copy(e, k))

    @pl.loop(bulk - lag, bulk - 1)
    def _(e):
        settle_both(e)

    @pl.when(odd)
    def _():
        each_late(lambda copy: copy.start())

    settle_both(bulk - 1)

    for k in range(1, n):
        zero_copy(k).wait()

    @pl.loop(bulk - slots, bulk)
    def _(e):
        drain(lax.rem(e, slots))

    @pl.when(odd)
    def _():
        each_late(lambda copy: copy.wait())


def cross(
    n, done, late, early, bulk_gate, bulk_up, final, scale_gate, scale_up,
    wide, send_sem, recv_sem, go_sem,
):
    experts, rows = late.shape[1], late.shape[4]
    me = lax.axis_index("zero")
    odd = lax.rem(me, 2) == 1
    first = bulk_gate.shape[0] - experts

    last = experts - 1

    def place(source, e):
        return final.at[e, :, :, pl.ds(pl.multiple_of(source * rows, rows), rows)]

    def copy(e, k, half=None):
        peer = lax.rem(me + k, n)
        row = e if half is None else e + half

        def part_of(ref):
            return ref if half is None else ref.at[half]

        return pltpu.make_async_remote_copy(
            src_ref=part_of(late.at[peer, e]),
            dst_ref=part_of(place(me, e)),
            send_sem=send_sem.at[row, k],
            recv_sem=recv_sem.at[row, k],
            **at("zero", peer),
        )

    def each(start, act):
        @pl.loop(0, last)
        def _(e):
            for k in range(start, n, 2):
                act(copy(e, k))

        for half in range(2):
            for k in range(start, n, 2):
                act(copy(last, k, half))

    def step(e, halves):
        for half, scale in enumerate((scale_gate, scale_up)):

            def block(k):
                return place(lax.rem(me - k + n, n), e).at[half]

            def arrive(k):
                source = lax.rem(me - k + n, n)
                arrived = block(k) if halves else place(source, e)

                def landed():
                    pltpu.make_async_remote_copy(
                        src_ref=arrived,
                        dst_ref=arrived,
                        send_sem=send_sem.at[0, 0],
                        recv_sem=recv_sem.at[e + half, k],
                        **at("zero", source),
                    ).wait_recv()

                if halves or half == 0:
                    if k % 2:
                        landed()
                    elif k:
                        pl.when(jnp.logical_not(odd))(landed)

            settle(n, block, arrive, wide, scale, first + e)

    barrier = pltpu.get_barrier_semaphore()

    @pl.when(jnp.logical_not(odd))
    def _():
        for k in range(2, n, 2):
            pl.semaphore_signal(barrier, inc=1, **at("zero", lax.rem(me + k, n)))
        pl.semaphore_wait(barrier, n // 2 - 1)
        each(2, lambda c: c.start())
        for k in range(1, n, 2):
            pl.semaphore_signal(barrier, inc=1, **at("zero", lax.rem(me + k, n)))

    @pl.when(odd)
    def _():
        pl.semaphore_wait(barrier, n // 2)
        for k in range(1, n, 2):
            pl.semaphore_signal(go_sem, inc=1, **at("zero", lax.rem(me + k, n)))

    def own():
        scale_gate[...] = bulk_gate[...]
        scale_up[...] = bulk_up[...]

        @pl.loop(0, experts)
        def _(e):
            place(me, e)[...] = late[me, e]

    @pl.when(jnp.logical_not(odd))
    def _():
        own()
        pl.semaphore_wait(go_sem, n // 2)

    @pl.when(odd)
    def _():
        own()

        @pl.loop(0, experts)
        def _(e):
            for k in range(2, n, 2):
                source = lax.rem(me - k + n, n)
                place(source, e)[...] = early[source // 2, e]

    each(1, lambda c: c.start())

    @pl.loop(0, last)
    def _(e):
        step(e, False)

    step(last, True)

    each(1, lambda c: c.wait_send())

    @pl.when(jnp.logical_not(odd))
    def _():
        each(2, lambda c: c.wait_send())


def copy_out(source, outs, first, sem):
    n, count, _, _, rows = source.shape
    return [
        pltpu.make_async_copy(
            source.at[s, :, half],
            out.at[first : first + count, :, s * rows : (s + 1) * rows],
            sem.at[s, half],
        )
        for s in range(n)
        for half, out in enumerate(outs)
    ]


def run(copies):
    for copy in copies:
        copy.start()
    for copy in copies:
        copy.wait()


def finish_bulk(recv, router, ready_gate, ready_up, router_out, done, sem, router_sem):
    done[...] = jnp.zeros_like(done)
    copies = copy_out(recv, (ready_gate, ready_up), 0, sem)
    run(copies + [pltpu.make_async_copy(router, router_out, router_sem)])


def finish_rest(
    final, scale_gate, scale_up, gate_in, up_in, ready_gate, ready_up, scale_gate_out, scale_up_out, sem, scale_sem,
):
    count = final.shape[0]
    first = ready_gate.shape[0] - count
    copies = [
        pltpu.make_async_copy(final.at[e, half], out.at[first + e], sem.at[e, half])
        for e in range(count)
        for half, out in enumerate((ready_gate, ready_up))
    ]
    copies.append(pltpu.make_async_copy(scale_gate, scale_gate_out, scale_sem.at[0]))
    copies.append(pltpu.make_async_copy(scale_up, scale_up_out, scale_sem.at[1]))
    run(copies)


def solution(mesh):
    n, nb = mesh.shape["zero"], mesh.shape["bank"]

    def local(train_gate, train_up, router_weight, router_gain):
        experts, rows, cols = train_gate.shape
        width = cols // n
        d_model = rows * n
        mine = router_weight.shape[1]
        rest = min(max(round(experts * TAIL), 1), experts - 1)
        bulk = experts - rest
        slots = min(SLOTS, bulk)
        hbm = pl.BlockSpec(memory_space=pltpu.HBM)
        inside = pl.BlockSpec(memory_space=pltpu.VMEM)
        padded = -(-width // LANES) * LANES
        scale = jax.ShapeDtypeStruct((experts, width), jnp.float32)
        joined = jax.ShapeDtypeStruct((nb, mine, d_model), jnp.bfloat16)

        def blocks(sources, count):
            return jax.ShapeDtypeStruct((sources, count, 2, width, rows), jnp.bfloat16)

        recv, router, bulk_gate, bulk_up, late, early = pl.pallas_call(
            functools.partial(exchange, n, nb),
            out_shape=(blocks(n, bulk), joined, scale, scale, blocks(n, rest), blocks(n // 2, rest)),
            in_specs=[hbm] * 4,
            out_specs=(inside,) * 6,
            scratch_shapes=[
                pltpu.VMEM((2, rows, cols), jnp.float32),
                pltpu.VMEM((cols, rows), jnp.float32),
                pltpu.VMEM((slots, n, 2, width, rows), jnp.bfloat16),
                pltpu.VMEM((mine, rows), jnp.bfloat16),
                pltpu.VMEM((padded, LANES), jnp.float32),
                pltpu.VMEM((mine, rows), jnp.float32),
                pltpu.VMEM((1, rows), jnp.float32),
                pltpu.SemaphoreType.DMA((2,)),
                pltpu.SemaphoreType.DMA((2,)),
                pltpu.SemaphoreType.DMA((slots, n)),
                pltpu.SemaphoreType.DMA((bulk, n)),
                pltpu.SemaphoreType.DMA((rest, n)),
                pltpu.SemaphoreType.DMA((rest, n)),
                pltpu.SemaphoreType.DMA((nb,)),
                pltpu.SemaphoreType.DMA((nb,)),
                pltpu.SemaphoreType.DMA((n,)),
                pltpu.SemaphoreType.DMA((n,)),
                pltpu.SemaphoreType.REGULAR,
                pltpu.SemaphoreType.REGULAR,
            ],
            compiler_params=pltpu.CompilerParams(
                collective_id=0, has_side_effects=True, vmem_limit_bytes=EXCHANGE_VMEM
            ),
        )(
            train_gate,
            train_up,
            pltpu.with_memory_space_constraint(router_weight.T, pltpu.HBM),
            pltpu.with_memory_space_constraint(router_gain[None, :], pltpu.HBM),
        )

        ready = jax.ShapeDtypeStruct((experts, width, d_model), jnp.bfloat16)
        ready_gate, ready_up, router, done = pl.pallas_call(
            finish_bulk,
            out_shape=(ready, ready, joined, jax.ShapeDtypeStruct((8, LANES), jnp.float32)),
            in_specs=[inside] * 2,
            out_specs=(hbm,) * 3 + (inside,),
            scratch_shapes=[pltpu.SemaphoreType.DMA((n, 2)), pltpu.SemaphoreType.DMA],
            compiler_params=pltpu.CompilerParams(vmem_limit_bytes=FINISH_VMEM),
        )(recv, router)

        final, scale_gate, scale_up = pl.pallas_call(
            functools.partial(cross, n),
            out_shape=(jax.ShapeDtypeStruct((rest, 2, width, d_model), jnp.bfloat16), scale, scale),
            in_specs=[inside] * 5,
            out_specs=(inside,) * 3,
            scratch_shapes=[
                pltpu.VMEM((padded, LANES), jnp.float32),
                pltpu.SemaphoreType.DMA((rest + 1, n)),
                pltpu.SemaphoreType.DMA((rest + 1, n)),
                pltpu.SemaphoreType.REGULAR,
            ],
            compiler_params=pltpu.CompilerParams(
                collective_id=1, has_side_effects=True, vmem_limit_bytes=CROSS_VMEM
            ),
        )(done, late, early, bulk_gate, bulk_up)

        ready_gate, ready_up, scale_gate, scale_up = pl.pallas_call(
            finish_rest,
            out_shape=(ready, ready, scale, scale),
            in_specs=[inside] * 3 + [hbm] * 2,
            out_specs=(hbm,) * 4,
            input_output_aliases={3: 0, 4: 1},
            scratch_shapes=[pltpu.SemaphoreType.DMA((rest, 2)), pltpu.SemaphoreType.DMA((2,))],
            compiler_params=pltpu.CompilerParams(vmem_limit_bytes=FINISH_VMEM),
        )(final, scale_gate, scale_up, ready_gate, ready_up)
        return (
            jnp.swapaxes(ready_gate, 1, 2),
            jnp.swapaxes(ready_up, 1, 2),
            scale_gate,
            scale_up,
            router.reshape(nb * mine, d_model).T,
        )

    in_specs = (P("bank", "zero", None), P("bank", "zero", None), P("zero", "bank"), P("zero"))
    out_specs = (
        P("bank", None, "zero"),
        P("bank", None, "zero"),
        P("bank", "zero"),
        P("bank", "zero"),
        P(),
    )
    return jax.shard_map(local, mesh=mesh, in_specs=in_specs, out_specs=out_specs, check_vma=False)
```
